32 devices in a mesh: seq: 4 (over z), chan: 8 (over y, x, core).
Axes of the slice: x: 2, y: 2, z: 4, core: 2. Of those that a mesh axis runs over, the one named last changes fastest.
Arguments:
- tokens: bfloat16 [4096, 4096], P('seq', 'chan'), may hold values from -8 to 8
- norm_gain: float32 [4096], replicated, may hold values from 0.5 to 1.5
- gate_proj: bfloat16 [4096, 8192], P(None, 'chan'), may hold values from -0.09375 to 0.09375
- inner_proj: bfloat16 [4096, 8192], P(None, 'chan'), may hold values from -0.09375 to 0.09375
- state_proj: bfloat16 [4096, 384], P('chan'), may hold values from -0.11816406 to 0.11816406
- conv_inner: float32 [4, 8192], P(None, 'chan'), may hold values from -3 to 3
- conv_state: float32 [4, 256], replicated, may hold values from -3 to 3
- log_rate: float32 [128], P('chan'), may hold values from -1 to 0
- rate_bias: float32 [128], P('chan'), may hold values from -16 to -2
- skip_gain: float32 [128], P('chan'), may hold values from 0.2 to 4
- gate_gain: float32 [8192], P('chan'), may hold values from 0.5 to 1.5
- out_proj: bfloat16 [8192, 4096], P('chan'), may hold values from -0.09375 to 0.09375
Outputs:
- layer_out: bfloat16 [4096, 4096], P('seq', 'chan')
The draws below stay inside these ranges and needn't reach their ends.
All inputs are finite; a program needn't handle non-finite values.
Results may differ from the reference program's by a relative error of at most 0.012.
Values may be sent and summed in bfloat16 or wider, within the bound.
A program may use at most 128 MiB of HBM per device.

```python
import jax
import jax.numpy as jnp
from jax import lax

D = 4096
H = 128
P_SIZE = 64
N = 128
K = 4
Q = 256
DI = 8192
TOKENS = 4096


def layout_plan(key):
    base_key = jax.random.fold_in(key, 4211)
    direction = jnp.clip(jax.random.normal(jax.random.fold_in(base_key, 1), (D,), jnp.float32), -6.0, 6.0)
    spot_count = max(4, TOKENS // 512)
    spot_rows = jax.random.randint(jax.random.fold_in(base_key, 2), (spot_count,), 0, TOKENS)
    spot_power = jax.random.uniform(jax.random.fold_in(base_key, 5), (spot_count,), jnp.float32, 0.8, 1.0)
    mixing = jax.random.uniform(jax.random.fold_in(base_key, 3), (H,), jnp.float32)
    memory = 30.0 * jnp.exp(mixing * jnp.log(jnp.float32(2 * TOKENS)))
    rate_logs = jax.random.uniform(jax.random.fold_in(base_key, 4), (H,), jnp.float32, -1.0, 0.0)
    offset = -jnp.log(1.65 * jnp.exp(rate_logs) * memory)
    return (direction, spot_rows, spot_power, rate_logs, offset)


def draw_tokens(key, part):
    direction, spot_rows, spot_power, rate_logs, offset = layout_plan(key)
    grid_key = jax.random.fold_in(key, 11)
    noise_draw = jnp.clip(jax.random.normal(grid_key, (TOKENS, D), jnp.float32), -6.0, 6.0)
    hits = jnp.arange(TOKENS)[:, None] == spot_rows[None, :]
    marked = jnp.any(hits, axis=1)
    power = jnp.max(jnp.where(hits, spot_power[None, :], 0.0), axis=1)
    result = jnp.where(marked[:, None], power[:, None] * direction[None, :] + 0.3 * noise_draw, noise_draw)
    return result.astype(jnp.bfloat16)


def draw_state_proj(key, part):
    direction, spot_rows, spot_power, rate_logs, offset = layout_plan(key)
    noise_draw = jnp.clip(jax.random.normal(jax.random.fold_in(key, 12), (D, 2 * N + H), jnp.float32), -6.0, 6.0)
    noise_draw = noise_draw / jnp.sqrt(jnp.float32(D))
    push_cols = jnp.concatenate([jnp.zeros((2 * N,), jnp.float32), -offset])
    return (noise_draw + direction[:, None] * push_cols[None, :] / D).astype(jnp.bfloat16)


def draw_log_rate(key, part):
    direction, spot_rows, spot_power, rate_logs, offset = layout_plan(key)
    return rate_logs


def draw_rate_bias(key, part):
    direction, spot_rows, spot_power, rate_logs, offset = layout_plan(key)
    return offset


def draw_skip_gain(key, part):
    base_key = jax.random.fold_in(key, 13)
    height = jnp.arange(H, dtype=jnp.float32) / H
    spread = jnp.exp(jax.random.uniform(base_key, (H,), jnp.float32, -0.35, 0.35))
    return (0.5 + 2.0 * height) * spread


def spiked(values, own_key, source, target, shards_of, factor):
    owner, partner = [(jnp.arange(values.shape[position]) // (values.shape[position] // shards_of)).reshape([-1 if axis == position else 1 for axis in range(values.ndim)]) for position in (source, target)]
    chosen = jax.random.permutation(own_key, shards_of)[partner]
    strong = (owner == chosen) | (owner == (partner + shards_of // 2) % shards_of)
    return jnp.where(strong, factor * values, values)


def block_scale(key, dims, cuts, least, largest):
    def one(position, parts):
        heights = jax.random.uniform(jax.random.fold_in(jax.random.fold_in(key, 6), position), (parts,), jnp.float32, least / len(cuts), largest / len(cuts))
        return jnp.repeat(jnp.exp(heights), dims[position] // parts).reshape((-1,) + (1,) * (len(dims) - position - 1))

    factor_of = one(*cuts[0])
    for cut in cuts[1:]:
        factor_of = factor_of * one(*cut)
    return factor_of


def normal_values(key, shape, scale, limit, shards=(), kind=jnp.bfloat16):
    factor_of = block_scale(key, shape, shards, -0.22, 0.18) if shards else 1.0
    values = jax.random.normal(key, shape, jnp.float32) * scale * factor_of
    return jnp.minimum(jnp.maximum(values, -limit), limit).astype(kind)


def noise_with(own_key, dims, scale, bound, cuts, heavy, held_as=jnp.bfloat16):
    values = scale * jax.random.normal(own_key, dims, jnp.float32)
    if cuts:
        values = values * block_scale(own_key, dims, cuts, -0.22, 0.18)
    return jnp.clip(spiked(values, jax.random.fold_in(own_key, 3), *heavy), -bound, bound).astype(held_as)


def setup_inputs(seed: int = 0) -> dict:
    key_list = jax.random.split(jax.random.key(seed), 13)
    return {
        "tokens": draw_tokens(jax.random.fold_in(key_list[12], 71), 0),
        "norm_gain": jnp.clip(1.0 + 0.1 * jax.random.normal(key_list[1], (D,), jnp.float32), 0.5, 1.5),
        "gate_proj": normal_values(key_list[2], (D, DI), D ** -0.5, 0.09375, ((1, 8),)),
        "inner_proj": normal_values(key_list[3], (D, DI), D ** -0.5, 0.09375, ((1, 8),)),
        "state_proj": draw_state_proj(jax.random.fold_in(key_list[12], 71), 0),
        "conv_inner": normal_values(key_list[5], (K, DI), K ** -0.5, 3.0, ((1, 8),), jnp.float32),
        "conv_state": normal_values(key_list[6], (K, 2 * N), K ** -0.5, 3.0, (), jnp.float32),
        "log_rate": draw_log_rate(jax.random.fold_in(key_list[12], 71), 0),
        "rate_bias": draw_rate_bias(jax.random.fold_in(key_list[12], 71), 0),
        "skip_gain": draw_skip_gain(jax.random.fold_in(key_list[12], 71), 0),
        "gate_gain": jnp.clip(1.0 + 0.1 * jax.random.normal(key_list[10], (DI,), jnp.float32), 0.5, 1.5),
        "out_proj": noise_with(key_list[11], (DI, D), DI ** -0.5, 0.09375, ((0, 8),), (0, 1, 8, 2.0)),
    }


precise = lax.Precision.HIGHEST

def causal_mix(fresh_rows, weights):
    length = fresh_rows.shape[0]
    padded = jnp.concatenate([jnp.zeros((K - 1, fresh_rows.shape[1]), fresh_rows.dtype), fresh_rows], axis=0)
    summed = jnp.zeros(fresh_rows.shape, jnp.float32)
    for offset in range(K):
        summed = summed + weights[offset] * padded[offset:offset + length].astype(jnp.float32)
    return jax.nn.silu(summed)

def block_step(state, pieces):
    values, in_map, out_map, step_size, decay_log = pieces
    within = jnp.cumsum(decay_log, axis=0)
    log_gaps = within[:, None, :] - within[None, :, :]
    lower_mask = jnp.arange(Q)[:, None] >= jnp.arange(Q)[None, :]
    fading = jnp.exp(jnp.where(lower_mask[:, :, None], log_gaps, -jnp.inf))
    scores = jnp.dot(out_map, in_map.T, precision=precise)
    mixing = scores[:, :, None] * fading * step_size[None, :, :]
    inside = jnp.einsum('tsh,shp->thp', mixing, values, precision=precise)
    carried = jnp.einsum('tn,hnp->thp', out_map, state, precision=precise) * jnp.exp(within)[:, :, None]
    tail_weight = jnp.exp(within[-1:] - within) * step_size
    fresh_state = jnp.einsum('sn,shp->hnp', in_map, values * tail_weight[:, :, None], precision=precise)
    state = jnp.exp(within[-1])[:, None, None] * state + fresh_state
    return (state, inside + carried)

def reference(tokens, norm_gain, gate_proj, inner_proj, state_proj, conv_inner, conv_state, log_rate, rate_bias, skip_gain, gate_gain, out_proj):
    widened = tokens.astype(jnp.float32)
    inverse = lax.rsqrt(lax.optimization_barrier(jnp.mean(widened * widened, axis=1, keepdims=True)) + 1e-05)
    normed = (widened * inverse * norm_gain).astype(jnp.bfloat16)
    gate_raw = jnp.dot(normed, gate_proj, preferred_element_type=jnp.float32).astype(jnp.bfloat16)
    inner_raw = jnp.dot(normed, inner_proj, preferred_element_type=jnp.float32).astype(jnp.bfloat16)
    projected = jnp.dot(normed, state_proj, preferred_element_type=jnp.float32)
    state_raw = projected[:, :2 * N]
    raw_rate = projected[:, 2 * N:]
    inner_conv = causal_mix(inner_raw, conv_inner)
    state_conv = causal_mix(state_raw, conv_state)
    step_size = jax.nn.softplus(raw_rate + rate_bias)
    decay_log = -jnp.exp(log_rate) * step_size
    blocks = TOKENS // Q
    pieces = (inner_conv.reshape(blocks, Q, H, P_SIZE), state_conv[:, :N].reshape(blocks, Q, N), state_conv[:, N:].reshape(blocks, Q, N), step_size.reshape(blocks, Q, H), decay_log.reshape(blocks, Q, H))
    start_state = jnp.zeros((H, N, P_SIZE), jnp.float32)
    final_state, ssd_parts = lax.scan(block_step, start_state, pieces)
    skip_wide = jnp.repeat(skip_gain, P_SIZE)
    ssd_out = ssd_parts.reshape(TOKENS, DI) + skip_wide * inner_conv
    gated_out = ssd_out * jax.nn.silu(gate_raw.astype(jnp.float32))
    norm_scale = lax.rsqrt(lax.optimization_barrier(jnp.mean(gated_out * gated_out, axis=1, keepdims=True)) + 1e-05)
    shaped = (gated_out * norm_scale * gate_gain).astype(jnp.bfloat16)
    added = jnp.dot(shaped, out_proj, preferred_element_type=jnp.float32)
    return (widened + added).astype(jnp.bfloat16)
```

```python
import jax
import jax.numpy as jnp
from jax import lax
from jax.experimental import pallas as pl
from jax.experimental.pallas import tpu as pltpu
from jax.sharding import PartitionSpec as P

P_SIZE = 64
N = 128
K = 4
Q = 256
LANES = 2 * P_SIZE
RIM = 8

f32, bf16 = jnp.float32, jnp.bfloat16


def from_behind(value, axis, steps):
    count = lax.axis_size(axis)
    leading, last = (max(0, -steps), min(count, count - steps))
    return lax.ppermute(value, axis, [(source, source + steps) for source in range(leading, last)])


def wide_pair(columns, pair):
    rows = columns.shape[0]
    lane = lax.broadcasted_iota(jnp.int32, (rows, LANES), 1)
    first = jnp.broadcast_to(columns[:, 2 * pair : 2 * pair + 1], (rows, LANES))
    second = jnp.broadcast_to(columns[:, 2 * pair + 1 : 2 * pair + 2], (rows, LANES))
    return jnp.where(lane < P_SIZE, first, second)


def scan_kernel(
    inner_ref, inner_rim_ref, state_ref, state_rim_ref, step_ref, step_t_ref, rate_ref, rate_t_ref,
    conv_inner_ref, conv_state_ref, skip_ref,
    y_ref, out_map_ref, log_ref, end_ref, fade_ref,
    held, state_ext, inner_ext, total,
):
    block = pl.program_id(0)
    heads = step_ref.shape[1]

    @pl.when(block == 0)
    def _():
        held[...] = jnp.zeros_like(held)
        total[...] = jnp.zeros_like(total)
        state_ext[0:RIM] = state_rim_ref[...]
        inner_ext[0:RIM] = inner_rim_ref[...]

    state_ext[RIM : RIM + Q] = state_ref[...]
    inner_ext[RIM : RIM + Q] = inner_ref[...].astype(f32)

    def mixed(ext, taps, lanes):
        summed = taps[0:1, lanes] * ext[RIM - 3 : RIM - 3 + Q, lanes]
        for offset in range(1, K):
            start = RIM - (K - 1) + offset
            summed = summed + taps[offset : offset + 1, lanes] * ext[start : start + Q, lanes]
        return summed * (1.0 / (1.0 + jnp.exp(-summed)))

    in_map = mixed(state_ext, conv_state_ref, slice(0, N))
    out_map = mixed(state_ext, conv_state_ref, slice(N, 2 * N)).astype(bf16)
    out_map_ref[...] = out_map
    in_map_t = jnp.transpose(in_map).astype(bf16)

    row = lax.broadcasted_iota(jnp.int32, (Q, Q), 0)
    column = lax.broadcasted_iota(jnp.int32, (Q, Q), 1)
    lower = row >= column
    scores = jnp.dot(out_map, in_map_t, preferred_element_type=f32)
    scores = jnp.where(lower, scores, 0.0)
    step = step_ref[...]
    logs = rate_ref[...] * step
    logs_t = rate_t_ref[...] * step_t_ref[...]
    within = jnp.dot(
        lower.astype(f32), logs, precision=lax.Precision.HIGHEST, preferred_element_type=f32
    )
    within_t = jnp.dot(
        logs_t, (row <= column).astype(f32), precision=lax.Precision.HIGHEST,
        preferred_element_type=f32,
    )
    log_ref[...] = within + total[...]
    last = within[Q - 1 : Q]
    grown = jnp.exp(within)
    tail = jnp.exp(last - within) * step
    block_fade = jnp.exp(last)
    lane = lax.broadcasted_iota(jnp.int32, (Q, LANES), 1)
    for pair in range(heads // 2):
        lanes = slice(pair * LANES, (pair + 1) * LANES)
        x = mixed(inner_ext, conv_inner_ref, lanes)
        stepped = (x * wide_pair(step, pair)).astype(bf16)
        parts = []
        for head in (2 * pair, 2 * pair + 1):
            gap = within[:, head : head + 1] - within_t[head : head + 1, :]
            mixing = (scores * jnp.exp(jnp.minimum(gap, 0.0))).astype(bf16)
            parts.append(jnp.dot(mixing, stepped, preferred_element_type=f32))
        inside = jnp.where(lane < P_SIZE, parts[0], parts[1])
        before = held[:, lanes]
        carried = jnp.dot(out_map, before.astype(bf16), preferred_element_type=f32)
        y_ref[:, lanes] = inside + carried * wide_pair(grown, pair) + skip_ref[:, lanes] * x
        tailed = (x * wide_pair(tail, pair)).astype(bf16)
        fresh = jnp.dot(in_map_t, tailed, preferred_element_type=f32)
        held[:, lanes] = wide_pair(block_fade, pair) * before + fresh
    total[...] = total[...] + last
    end_ref[...] = held[...]
    fade_ref[...] = jnp.exp(total[...])
    state_ext[0:RIM] = state_ext[Q : Q + RIM]
    inner_ext[0:RIM] = inner_ext[Q : Q + RIM]


def local_scan(inner_raw, inner_rim, state_raw, state_rim, step, rate, conv_inner, conv_state, skip_wide):
    rows, width = inner_raw.shape
    heads = step.shape[1]

    def whole(shape):
        return pl.BlockSpec(shape, lambda c: (0, 0))

    return pl.pallas_call(
        scan_kernel,
        grid=(rows // Q,),
        in_specs=[
            pl.BlockSpec((Q, width), lambda c: (c, 0)),
            whole((RIM, width)),
            pl.BlockSpec((Q, 2 * N), lambda c: (c, 0)),
            whole((RIM, 2 * N)),
            pl.BlockSpec((Q, heads), lambda c: (c, 0)),
            pl.BlockSpec((heads, Q), lambda c: (0, c)),
            whole((1, heads)),
            whole((heads, 1)),
            whole((K, width)),
            whole((K, 2 * N)),
            whole((1, width)),
        ],
        out_specs=[
            pl.BlockSpec((Q, width), lambda c: (c, 0)),
            pl.BlockSpec((Q, N), lambda c: (c, 0)),
            pl.BlockSpec((Q, heads), lambda c: (c, 0)),
            whole((N, width)),
            whole((1, heads)),
        ],
        out_shape=[
            jax.ShapeDtypeStruct((rows, width), f32),
            jax.ShapeDtypeStruct((rows, N), bf16),
            jax.ShapeDtypeStruct((rows, heads), f32),
            jax.ShapeDtypeStruct((N, width), f32),
            jax.ShapeDtypeStruct((1, heads), f32),
        ],
        scratch_shapes=[
            pltpu.VMEM((N, width), f32),
            pltpu.VMEM((RIM + Q, 2 * N), f32),
            pltpu.VMEM((RIM + Q, width), f32),
            pltpu.VMEM((1, heads), f32),
        ],
        compiler_params=pltpu.CompilerParams(dimension_semantics=("arbitrary",)),
        cost_estimate=pl.CostEstimate(
            flops=rows * width * Q * 4, bytes_accessed=rows * width * 8, transcendentals=rows * heads * Q
        ),
    )(
        inner_raw, inner_rim, state_raw, state_rim, step, step.T, rate[None, :], rate[:, None],
        conv_inner, conv_state, skip_wide,
    )


def finish_kernel(y_ref, gate_ref, out_map_ref, log_ref, carried_ref, gain_ref, shaped_ref, energy_ref):
    heads = log_ref.shape[1]
    grown = jnp.exp(log_ref[...])
    out_map = out_map_ref[...]
    energy = jnp.zeros((Q, LANES), f32)
    for pair in range(heads // 2):
        lanes = slice(pair * LANES, (pair + 1) * LANES)
        carried = jnp.dot(out_map, carried_ref[:, lanes], preferred_element_type=f32)
        y = y_ref[:, lanes] + carried * wide_pair(grown, pair)
        gate = gate_ref[:, lanes].astype(f32)
        gated = y * (gate * (1.0 / (1.0 + jnp.exp(-gate))))
        energy = energy + gated * gated
        shaped_ref[:, lanes] = (gated * gain_ref[:, lanes]).astype(bf16)
    energy_ref[...] = jnp.sum(energy, axis=1, keepdims=True)


def finish(y, gate_raw, out_map, logs, carried, gate_gain):
    rows, width = y.shape
    heads = logs.shape[1]

    def rowwise(columns):
        return pl.BlockSpec((Q, columns), lambda c: (c, 0))

    return pl.pallas_call(
        finish_kernel,
        grid=(rows // Q,),
        in_specs=[
            rowwise(width),
            rowwise(width),
            rowwise(N),
            rowwise(heads),
            pl.BlockSpec((N, width), lambda c: (0, 0)),
            pl.BlockSpec((1, width), lambda c: (0, 0)),
        ],
        out_specs=[rowwise(width), rowwise(1)],
        out_shape=[
            jax.ShapeDtypeStruct((rows, width), bf16),
            jax.ShapeDtypeStruct((rows, 1), f32),
        ],
        compiler_params=pltpu.CompilerParams(dimension_semantics=("arbitrary",)),
        cost_estimate=pl.CostEstimate(
            flops=rows * width * N * 2, bytes_accessed=rows * width * 8, transcendentals=rows * width
        ),
    )(y, gate_raw, out_map, logs, carried, gate_gain)


def local(
    tokens,
    norm_gain,
    gate_proj,
    inner_proj,
    state_proj,
    conv_inner,
    conv_state,
    log_rate,
    rate_bias,
    skip_gain,
    gate_gain,
    out_proj,
):
    token_rows = tokens.shape[0]
    together = jnp.concatenate([tokens, state_proj.T], axis=0)
    together = lax.all_gather(together, "chan", axis=1, tiled=True)
    gathered, state_proj_t = together[:token_rows], together[token_rows:]
    widened = gathered.astype(f32)
    inverse = lax.rsqrt(jnp.mean(widened * widened, axis=1, keepdims=True) + 1e-05)
    normed = (widened * inverse * norm_gain).astype(bf16)
    projected = lax.dot_general(
        normed, state_proj_t, (((1,), (1,)), ((), ())), preferred_element_type=f32
    )
    inner_raw = jnp.dot(normed, inner_proj, preferred_element_type=f32).astype(bf16)
    gate_raw = jnp.dot(normed, gate_proj, preferred_element_type=f32).astype(bf16)
    heads = log_rate.shape[0]
    start_head = lax.axis_index("chan") * heads
    state_raw = projected[:, : 2 * N]
    raw_rate = lax.dynamic_slice_in_dim(projected, 2 * N + start_head, heads, 1)
    step = jax.nn.softplus(raw_rate + rate_bias)
    inner_rim = from_behind(inner_raw[-RIM:], "seq", 1).astype(f32)
    state_rim = from_behind(state_raw[-RIM:], "seq", 1)
    skip_wide = jnp.repeat(skip_gain, P_SIZE)[None, :]
    y, out_map, logs, device_end, device_fade = local_scan(
        inner_raw, inner_rim, state_raw, state_rim, step, -jnp.exp(log_rate),
        conv_inner, conv_state, skip_wide,
    )
    fade_wide = jnp.repeat(device_fade[0], P_SIZE)[None, :]
    carried = from_behind(device_end.astype(bf16), "seq", 1)
    for _ in range(lax.axis_size("seq") - 2):
        carried = from_behind((fade_wide * carried.astype(f32) + device_end).astype(bf16), "seq", 1)
    shaped, energy = finish(y, gate_raw, out_map, logs, carried, gate_gain[None, :])
    partial_out = jnp.dot(shaped, out_proj, preferred_element_type=f32).astype(bf16)
    summed = lax.psum_scatter(partial_out, "chan", scatter_dimension=1, tiled=True)
    channels = gate_gain.shape[0] * lax.axis_size("chan")
    norm_scale = lax.rsqrt(lax.psum(energy[:, 0], "chan") / channels + 1e-05)
    return (tokens.astype(f32) + summed.astype(f32) * norm_scale[:, None]).astype(bf16)


def solution(mesh):
    return jax.shard_map(
        local,
        mesh=mesh,
        in_specs=(
            P("seq", "chan"),
            P(),
            P(None, "chan"),
            P(None, "chan"),
            P("chan", None),
            P(None, "chan"),
            P(),
            P("chan"),
            P("chan"),
            P("chan"),
            P("chan"),
            P("chan", None),
        ),
        out_specs=P("seq", "chan"),
        check_vma=False,
    )
```

```python
import jax
import jax.numpy as jnp
from jax import lax
from jax.experimental import pallas as pl
from jax.experimental.pallas import tpu as pltpu
from jax.sharding import PartitionSpec as P

P_SIZE = 64
N = 128
K = 4
Q = 256
LANES = 2 * P_SIZE
RIM = 8
ROWS = 128

f32, bf16 = jnp.float32, jnp.bfloat16


def from_behind(value, axis, steps):
    count = lax.axis_size(axis)
    leading, last = (max(0, -steps), min(count, count - steps))
    return lax.ppermute(value, axis, [(source, source + steps) for source in range(leading, last)])


def wide_pair(columns, pair):
    rows = columns.shape[0]
    lane = lax.broadcasted_iota(jnp.int32, (rows, LANES), 1)
    first = jnp.broadcast_to(columns[:, 2 * pair : 2 * pair + 1], (rows, LANES))
    second = jnp.broadcast_to(columns[:, 2 * pair + 1 : 2 * pair + 2], (rows, LANES))
    return jnp.where(lane < P_SIZE, first, second)


def scan_kernel(
    inner_ref, inner_rim_ref, state_ref, state_rim_ref, step_ref, step_t_ref, rate_ref, rate_t_ref,
    conv_inner_ref, conv_state_ref, skip_ref,
    y_ref, out_map_ref, log_ref, end_ref, fade_ref,
    held, state_ext, inner_ext, total,
):
    block = pl.program_id(0)
    heads = step_ref.shape[1]

    @pl.when(block == 0)
    def _():
        held[...] = jnp.zeros_like(held)
        total[...] = jnp.zeros_like(total)
        state_ext[0:RIM] = state_rim_ref[...]
        inner_ext[0:RIM] = inner_rim_ref[...]

    state_ext[RIM : RIM + Q] = state_ref[...]
    inner_ext[RIM : RIM + Q] = inner_ref[...].astype(f32)

    def mixed(ext, taps, lanes):
        summed = taps[0:1, lanes] * ext[RIM - 3 : RIM - 3 + Q, lanes]
        for offset in range(1, K):
            start = RIM - (K - 1) + offset
            summed = summed + taps[offset : offset + 1, lanes] * ext[start : start + Q, lanes]
        return summed * (1.0 / (1.0 + jnp.exp(-summed)))

    in_map = mixed(state_ext, conv_state_ref, slice(0, N))
    out_map = mixed(state_ext, conv_state_ref, slice(N, 2 * N)).astype(bf16)
    out_map_ref[...] = out_map
    in_map_t = jnp.transpose(in_map).astype(bf16)

    row = lax.broadcasted_iota(jnp.int32, (Q, Q), 0)
    column = lax.broadcasted_iota(jnp.int32, (Q, Q), 1)
    lower = row >= column
    scores = jnp.dot(out_map, in_map_t, preferred_element_type=f32)
    scores = jnp.where(lower, scores, 0.0)
    step = step_ref[...]
    logs = rate_ref[...] * step
    logs_t = rate_t_ref[...] * step_t_ref[...]
    within = jnp.dot(
        lower.astype(f32), logs, precision=lax.Precision.HIGHEST, preferred_element_type=f32
    )
    within_t = jnp.dot(
        logs_t, (row <= column).astype(f32), precision=lax.Precision.HIGHEST,
        preferred_element_type=f32,
    )
    log_ref[...] = within + total[...]
    last = within[Q - 1 : Q]
    grown = jnp.exp(within)
    tail = jnp.exp(last - within) * step
    block_fade = jnp.exp(last)
    lane = lax.broadcasted_iota(jnp.int32, (Q, LANES), 1)
    for pair in range(heads // 2):
        lanes = slice(pair * LANES, (pair + 1) * LANES)
        x = mixed(inner_ext, conv_inner_ref, lanes)
        stepped = (x * wide_pair(step, pair)).astype(bf16)
        parts = []
        for head in (2 * pair, 2 * pair + 1):
            gap = within[:, head : head + 1] - within_t[head : head + 1, :]
            mixing = (scores * jnp.exp(jnp.minimum(gap, 0.0))).astype(bf16)
            parts.append(jnp.dot(mixing, stepped, preferred_element_type=f32))
        inside = jnp.where(lane < P_SIZE, parts[0], parts[1])
        before = held[:, lanes]
        carried = jnp.dot(out_map, before.astype(bf16), preferred_element_type=f32)
        y_ref[:, lanes] = inside + carried * wide_pair(grown, pair) + skip_ref[:, lanes] * x
        tailed = (x * wide_pair(tail, pair)).astype(bf16)
        fresh = jnp.dot(in_map_t, tailed, preferred_element_type=f32)
        held[:, lanes] = wide_pair(block_fade, pair) * before + fresh
    total[...] = total[...] + last
    end_ref[...] = held[...]
    fade_ref[...] = jnp.exp(total[...])
    state_ext[0:RIM] = state_ext[Q : Q + RIM]
    inner_ext[0:RIM] = inner_ext[Q : Q + RIM]


def local_scan(inner_raw, inner_rim, state_raw, state_rim, step, rate, conv_inner, conv_state, skip_wide):
    rows, width = inner_raw.shape
    heads = step.shape[1]

    def whole(shape):
        return pl.BlockSpec(shape, lambda c: (0, 0))

    return pl.pallas_call(
        scan_kernel,
        grid=(rows // Q,),
        in_specs=[
            pl.BlockSpec((Q, width), lambda c: (c, 0)),
            whole((RIM, width)),
            pl.BlockSpec((Q, 2 * N), lambda c: (c, 0)),
            whole((RIM, 2 * N)),
            pl.BlockSpec((Q, heads), lambda c: (c, 0)),
            pl.BlockSpec((heads, Q), lambda c: (0, c)),
            whole((1, heads)),
            whole((heads, 1)),
            whole((K, width)),
            whole((K, 2 * N)),
            whole((1, width)),
        ],
        out_specs=[
            pl.BlockSpec((Q, width), lambda c: (c, 0)),
            pl.BlockSpec((Q, N), lambda c: (c, 0)),
            pl.BlockSpec((Q, heads), lambda c: (c, 0)),
            whole((N, width)),
            whole((1, heads)),
        ],
        out_shape=[
            jax.ShapeDtypeStruct((rows, width), f32),
            jax.ShapeDtypeStruct((rows, N), bf16),
            jax.ShapeDtypeStruct((rows, heads), f32),
            jax.ShapeDtypeStruct((N, width), f32),
            jax.ShapeDtypeStruct((1, heads), f32),
        ],
        scratch_shapes=[
            pltpu.VMEM((N, width), f32),
            pltpu.VMEM((RIM + Q, 2 * N), f32),
            pltpu.VMEM((RIM + Q, width), f32),
            pltpu.VMEM((1, heads), f32),
        ],
        compiler_params=pltpu.CompilerParams(dimension_semantics=("arbitrary",)),
        cost_estimate=pl.CostEstimate(
            flops=rows * width * Q * 4, bytes_accessed=rows * width * 8, transcendentals=rows * heads * Q
        ),
    )(
        inner_raw, inner_rim, state_raw, state_rim, step, step.T, rate[None, :], rate[:, None],
        conv_inner, conv_state, skip_wide,
    )


def finish_kernel(y_ref, gate_ref, late_gate_ref, out_map_ref, log_ref, carried_ref, gain_ref, shaped_ref, energy_ref):
    heads = log_ref.shape[1]
    early = pl.program_id(0) < pl.num_programs(0) // 2
    grown = jnp.exp(log_ref[...])
    out_map = out_map_ref[...]
    energy = jnp.zeros((Q, LANES), f32)
    for pair in range(heads // 2):
        lanes = slice(pair * LANES, (pair + 1) * LANES)
        carried = jnp.dot(out_map, carried_ref[:, lanes], preferred_element_type=f32)
        y = y_ref[:, lanes] + carried * wide_pair(grown, pair)
        gate = jnp.where(early, gate_ref[:, lanes].astype(f32), late_gate_ref[:, lanes].astype(f32))
        gated = y * (gate * (1.0 / (1.0 + jnp.exp(-gate))))
        energy = energy + gated * gated
        shaped_ref[:, lanes] = (gated * gain_ref[:, lanes]).astype(bf16)
    energy_ref[...] = jnp.sum(energy, axis=1, keepdims=True)


def finish(y, gates, out_map, logs, carried, gate_gain):
    rows, width = y.shape
    heads = logs.shape[1]
    middle = rows // Q // 2

    def rowwise(columns):
        return pl.BlockSpec((Q, columns), lambda c: (c, 0))

    return pl.pallas_call(
        finish_kernel,
        grid=(rows // Q,),
        in_specs=[
            rowwise(width),
            pl.BlockSpec((Q, width), lambda c: (jnp.minimum(c, middle - 1), 0)),
            pl.BlockSpec((Q, width), lambda c: (jnp.maximum(c - middle, 0), 0)),
            rowwise(N),
            rowwise(heads),
            pl.BlockSpec((N, width), lambda c: (0, 0)),
            pl.BlockSpec((1, width), lambda c: (0, 0)),
        ],
        out_specs=[rowwise(width), rowwise(1)],
        out_shape=[
            jax.ShapeDtypeStruct((rows, width), bf16),
            jax.ShapeDtypeStruct((rows, 1), f32),
        ],
        compiler_params=pltpu.CompilerParams(dimension_semantics=("arbitrary",)),
        cost_estimate=pl.CostEstimate(
            flops=rows * width * N * 2, bytes_accessed=rows * width * 8, transcendentals=rows * width
        ),
    )(y, gates[0], gates[1], out_map, logs, carried, gate_gain)


def norm_kernel(token_ref, state_proj_ref, gain_ref, normed_ref, projected_ref):
    widened = token_ref[...].astype(f32)
    square = jnp.mean(widened * widened, axis=1, keepdims=True)
    normed = (widened * lax.rsqrt(square + 1e-05) * gain_ref[...]).astype(bf16)
    normed_ref[...] = normed
    projected_ref[...] = lax.dot_general(
        normed, state_proj_ref[...], (((1,), (1,)), ((), ())), preferred_element_type=f32
    )


def norm_and_project(together, norm_gain, outputs):
    width = together.shape[1]
    rows = together.shape[0] - outputs
    skipped = outputs // ROWS
    return pl.pallas_call(
        norm_kernel,
        grid=(rows // ROWS,),
        in_specs=[
            pl.BlockSpec((ROWS, width), lambda c: (c + skipped, 0)),
            pl.BlockSpec((outputs, width), lambda c: (0, 0)),
            pl.BlockSpec((1, width), lambda c: (0, 0)),
        ],
        out_specs=[
            pl.BlockSpec((ROWS, width), lambda c: (c, 0)),
            pl.BlockSpec((ROWS, outputs), lambda c: (c, 0)),
        ],
        out_shape=[
            jax.ShapeDtypeStruct((rows, width), bf16),
            jax.ShapeDtypeStruct((rows, outputs), f32),
        ],
        compiler_params=pltpu.CompilerParams(dimension_semantics=("arbitrary",)),
        cost_estimate=pl.CostEstimate(
            flops=rows * width * outputs * 2, bytes_accessed=rows * width * 4, transcendentals=rows
        ),
    )(together, together, norm_gain[None, :])


def gate_part(normed, gate_proj, start, rows):
    return jnp.dot(normed[start : start + rows], gate_proj, preferred_element_type=f32).astype(bf16)


def local(
    tokens,
    norm_gain,
    gate_proj,
    inner_proj,
    state_proj,
    conv_inner,
    conv_state,
    log_rate,
    rate_bias,
    skip_gain,
    gate_gain,
    out_proj,
):
    token_rows = tokens.shape[0]
    outputs = state_proj.shape[1]
    together = jnp.concatenate([state_proj.T, tokens], axis=0)
    together = lax.all_gather(together, "chan", axis=1, tiled=True)
    normed, projected = norm_and_project(together, norm_gain, outputs)
    inner_raw = jnp.dot(normed, inner_proj, preferred_element_type=f32).astype(bf16)
    heads = log_rate.shape[0]
    start_head = lax.axis_index("chan") * heads
    state_raw = projected[:, : 2 * N]
    raw_rate = lax.dynamic_slice_in_dim(projected, 2 * N + start_head, heads, 1)
    step = jax.nn.softplus(raw_rate + rate_bias)
    inner_rim = from_behind(inner_raw[-RIM:], "seq", 1).astype(f32)
    state_rim = from_behind(state_raw[-RIM:], "seq", 1)
    skip_wide = jnp.repeat(skip_gain, P_SIZE)[None, :]
    y, out_map, logs, device_end, device_fade = local_scan(
        inner_raw, inner_rim, state_raw, state_rim, step, -jnp.exp(log_rate),
        conv_inner, conv_state, skip_wide,
    )
    fade_wide = jnp.repeat(device_fade[0], P_SIZE)[None, :]
    hops = lax.axis_size("seq") - 1
    half = token_rows // 2
    gates = []
    carried = from_behind(device_end.astype(bf16), "seq", 1)
    for hop in range(1, hops):
        onward = (fade_wide * carried.astype(f32) + device_end).astype(bf16)
        if hop >= hops - 1:
            gates.append(gate_part(normed, gate_proj, 0, half))
            onward, gates[0] = lax.optimization_barrier((onward, gates[0]))
        carried = from_behind(onward, "seq", 1)
    while len(gates) < 2:
        gates.append(gate_part(normed, gate_proj, len(gates) * half, half))
    shaped, energy = finish(y, gates, out_map, logs, carried, gate_gain[None, :])
    partial_out = jnp.dot(shaped, out_proj, preferred_element_type=f32).astype(bf16)
    summed = lax.psum_scatter(partial_out, "chan", scatter_dimension=1, tiled=True)
    channels = gate_gain.shape[0] * lax.axis_size("chan")
    norm_scale = lax.rsqrt(lax.psum(energy[:, 0], "chan") / channels + 1e-05)
    return (tokens.astype(f32) + summed.astype(f32) * norm_scale[:, None]).astype(bf16)


def solution(mesh):
    return jax.shard_map(
        local,
        mesh=mesh,
        in_specs=(
            P("seq", "chan"),
            P(),
            P(None, "chan"),
            P(None, "chan"),
            P("chan", None),
            P(None, "chan"),
            P(),
            P("chan"),
            P("chan"),
            P("chan"),
            P("chan"),
            P("chan", None),
        ),
        out_specs=P("seq", "chan"),
        check_vma=False,
    )
```
